128 devices in a mesh: tm: 32 (over y_hi, z, x), chan: 4 (over y_lo, core).
Axes of the slice: x: 4, y: 4 (y_hi: 2, y_lo: 2; y = y_hi * 2 + y_lo), z: 4, core: 2. Of those that a mesh axis runs over, the one named last changes fastest.
Arguments:
- fwd_in: bfloat16 [65536, 512], P('tm', 'chan'), may hold values from -28 to 28, as said below
- bwd_in: bfloat16 [65536, 512], P('tm', 'chan'), may hold values from -28 to 28, as said below
Outputs:
- forward_error: bfloat16 [65536, 512], P('tm', 'chan')
- backward_error: bfloat16 [65536, 512], P('tm', 'chan')
The draws below stay inside these ranges and needn't reach their ends.
Inputs may be any that keep to these rules, and one draw needn't show every extreme that they name: `fwd_in`: real-valued samples. `bwd_in`: real-valued samples.
All inputs are finite; a program needn't handle non-finite values.
Results may differ from the reference program's by a relative error of at most 0.0066.
Values may be sent and summed in bfloat16 or wider, within the bound.
A program may use at most 64 MiB of HBM per device.

```python
import math
import jax
import jax.numpy as jnp
from jax import lax

C = 512
TD = 2048
ORDERS = 2
NSTEPS = 6
SAMPLES = 65536


def error_pair(key):
    keys = jax.random.split(jax.random.fold_in(key, 17), 13)
    seg_rows = TD // 4
    seg_count = SAMPLES // seg_rows
    factor_series = jnp.clip(jax.random.normal(keys[10], (SAMPLES + 1, 3), jnp.float32), -4.0, 4.0)
    loadings = 0.15 * jax.random.normal(keys[11], (3, C), jnp.float32)
    shared = factor_series[:, 0:1] * loadings[0:1] + factor_series[:, 1:2] * loadings[1:2] + factor_series[:, 2:3] * loadings[2:3]
    lead = jnp.clip(jax.random.normal(keys[0], (SAMPLES + 1, C), jnp.float32), -4.0, 4.0) + shared
    own = 0.3 * jnp.clip(jax.random.normal(keys[1], (SAMPLES, C), jnp.float32), -4.0, 4.0)
    block_scale = jnp.exp(jax.random.uniform(keys[4], (seg_count, 1), jnp.float32, 0.0, math.log(10.0)))
    mix_sign = jnp.where(jax.random.uniform(keys[12], (), jnp.float32) < 0.5, -1.0, 1.0)
    block_mix = mix_sign * jax.random.uniform(keys[5], (seg_count, 1), jnp.float32, 0.6, 0.9)
    scale_rows = jnp.repeat(block_scale, seg_rows, axis=0)
    mix_rows = jnp.repeat(block_mix, seg_rows, axis=0)
    current = lead[:-1]
    earlier = jnp.concatenate([jnp.zeros((1, C), jnp.float32), current[:-1]], axis=0)
    base_fwd = current + 0.5 * earlier
    own_before = jnp.concatenate([jnp.zeros((1, C), jnp.float32), own[:-1]], axis=0)
    base_bwd = own + mix_rows * lead[1:] - 0.4 * own_before
    scale_fwd = jnp.exp(jax.random.uniform(keys[2], (1, C), jnp.float32, 0.0, math.log(3.2)))
    scale_bwd = jnp.exp(jax.random.uniform(keys[3], (1, C), jnp.float32, 0.0, math.log(3.2)))
    jitter_fwd = jnp.exp(jax.random.uniform(keys[8], (SAMPLES, 1), jnp.float32, 0.0, math.log(1.6)))
    jitter_bwd = jnp.exp(jax.random.uniform(keys[9], (SAMPLES, 1), jnp.float32, 0.0, math.log(1.6)))
    first = jnp.clip(base_fwd * scale_fwd * scale_rows * jitter_fwd / 6.0, -27.0, 27.0)
    second = jnp.clip(base_bwd * scale_bwd * scale_rows * jitter_bwd / 6.0, -27.0, 27.0)
    return (first, second)


def draw_fwd_in(key, part):
    first, second = error_pair(key)
    return first.astype(jnp.bfloat16)


def draw_bwd_in(key, part):
    first, second = error_pair(key)
    return second.astype(jnp.bfloat16)


def setup_inputs(seed: int = 0) -> dict:
    arg_keys = jax.random.split(jax.random.key(seed), 3)
    fwd_in = draw_fwd_in(jax.random.fold_in(arg_keys[2], 71), 0)
    bwd_in = draw_bwd_in(jax.random.fold_in(arg_keys[2], 71), 0)
    return {"fwd_in": fwd_in, "bwd_in": bwd_in}


def covariance(left, right):
    return jnp.dot(left.astype(jnp.float32).T, right.astype(jnp.float32), precision=lax.Precision.HIGHEST)

def newton_inverse(matrix):
    factor = lax.rsqrt(jnp.sum(matrix * matrix) + 1e-06)
    iterate = factor * jnp.eye(C, dtype=jnp.float32)
    for step in range(NSTEPS):
        product = jnp.dot(matrix, iterate, precision=lax.Precision.HIGHEST)
        iterate = 2.0 * iterate - jnp.dot(product, iterate, precision=lax.Precision.HIGHEST)
    return iterate

def reference(fwd_in, bwd_in):
    forward = fwd_in
    backward = bwd_in
    for order in range(ORDERS):
        shifted = jnp.concatenate([jnp.zeros((1, C), jnp.bfloat16), backward[:-1]], axis=0)
        cov_fwd = covariance(forward, forward)
        cov_bwd = covariance(shifted, shifted)
        cov_cross = covariance(forward, shifted)
        inv_fwd = newton_inverse(cov_fwd)
        inv_bwd = newton_inverse(cov_bwd)
        refl_fwd = (-jnp.dot(cov_cross, inv_bwd, precision=lax.Precision.HIGHEST)).astype(jnp.bfloat16)
        refl_bwd = (-jnp.dot(cov_cross.T, inv_fwd, precision=lax.Precision.HIGHEST)).astype(jnp.bfloat16)
        new_forward = forward.astype(jnp.float32) + jnp.dot(shifted.astype(jnp.float32), refl_fwd.astype(jnp.float32).T, precision=lax.Precision.HIGHEST)
        new_backward = shifted.astype(jnp.float32) + jnp.dot(forward.astype(jnp.float32), refl_bwd.astype(jnp.float32).T, precision=lax.Precision.HIGHEST)
        forward = new_forward.astype(jnp.bfloat16)
        backward = new_backward.astype(jnp.bfloat16)
    return (forward, backward)
```

```python
import jax
import jax.numpy as jnp
from jax import lax
from jax.experimental import pallas as pl
from jax.experimental.pallas import tpu as pltpu
from jax.sharding import PartitionSpec as P

ORDERS = 2
NSTEPS = 6
C = 512
W = 128
Q = 512
HALO = 16
BLK = 128
TRI = [(i, j) for i in range(4) for j in range(i, 4)]
ROWS = 18 * BLK
PART = ROWS // 3
CH1 = PART // 4
CH2 = CH1 // 4
HALF = 8 * BLK
MESH = pl.DeviceIdType.MESH
f32 = jnp.float32
bf16 = jnp.bfloat16
WIRE = f32


def dot_tn(a, b):
    return lax.dot_general(a, b, (((0,), (0,)), ((), ())), preferred_element_type=f32)


def dot_nt(a, b):
    return lax.dot_general(a, b, (((1,), (1,)), ((), ())), preferred_element_type=f32)


def dot_nn(a, b):
    return lax.dot_general(a, b, (((1,), (0,)), ((), ())), preferred_element_type=f32)


def kernel(
    fwd, bwd, out_f, out_b,
    fbuf, bbuf, wide, u, s1buf, s2buf, g1buf,
    d_send, d_recv, tot, p1, r1, acc1, p2, r2, acc2, p3, r3, fin, fin2,
    zq, amat, obuf,
    x_ssem, x_rsem, h_ssem, h_rsem, hl_sem, d_ssem, d_rsem, c_ssem, c_rsem, o_ssem, o_rsem,
):
    tm = lax.axis_index("tm")
    ch = lax.axis_index("chan")
    y_hi, zx = lax.div(tm, 16), lax.rem(tm, 16)
    z, x = lax.div(zx, 4), lax.rem(zx, 4)
    y_lo, core = lax.div(ch, 2), lax.rem(ch, 2)
    y = y_hi * 2 + y_lo
    partner = (tm, y_lo * 2 + 1 - core)

    def peer(axis, j):
        if axis == 0:
            return (tm - x + lax.rem(x + j, 4), ch)
        if axis == 1:
            ny = lax.rem(y + j, 4)
            return (lax.div(ny, 2) * 16 + zx, lax.rem(ny, 2) * 2 + core)
        return (y_hi * 16 + lax.rem(z + j, 4) * 4 + x, ch)

    pos = (x, y, z)
    nxt = lax.rem(tm + 1, 32)
    prv = lax.rem(tm + 31, 32)

    barrier = pltpu.get_barrier_semaphore()
    for j in (1, 2, 3):
        pl.semaphore_signal(barrier, inc=1, device_id=(tm, lax.rem(ch + j, 4)), device_id_type=MESH)
        for axis in range(3):
            pl.semaphore_signal(barrier, inc=1, device_id=peer(axis, j), device_id_type=MESH)

    @pl.when(ch == 0)
    def _():
        for k in range(4):
            pl.semaphore_signal(barrier, inc=1, device_id=(prv, k), device_id_type=MESH)

    pl.semaphore_wait(barrier, 13)

    def remote(src, dst, ssem, rsem, dev):
        return pltpu.make_async_remote_copy(
            src_ref=src, dst_ref=dst, send_sem=ssem, recv_sem=rsem, device_id=dev, device_id_type=MESH
        )

    mycols = pl.ds(pl.multiple_of(ch * W, W), W)
    myrows = pl.ds(pl.multiple_of(ch * Q, Q), Q)
    copies = []
    for a, (src, dst) in enumerate(((fwd, fbuf), (bwd, bbuf))):
        for j in (1, 2, 3):
            t = lax.rem(ch + j, 4)
            k = lax.rem(t + 3, 4)
            dev = (jnp.where(t == 0, nxt, tm), t)
            cp = remote(
                src.at[pl.ds(pl.multiple_of(k * Q + Q - HALO, HALO), HALO)],
                dst.at[pl.ds(0, HALO), mycols],
                h_ssem.at[a, j - 1], h_rsem.at[a, j - 1], dev,
            )
            cp.start()
            copies.append(cp)
    for j in (2, 1, 3):
        t = lax.rem(ch + j, 4)
        for a, (src, dst) in enumerate(((fwd, fbuf), (bwd, bbuf))):
            cp = remote(
                src.at[pl.ds(pl.multiple_of(t * Q, Q), Q)],
                dst.at[pl.ds(HALO, Q), mycols],
                x_ssem.at[a, j - 1], x_rsem.at[a, j - 1], (tm, t),
            )
            cp.start()
            copies.append(cp)

    @pl.when(ch == 0)
    def _():
        for a, (src, dst) in enumerate(((fwd, fbuf), (bwd, bbuf))):
            remote(
                src.at[pl.ds(4 * Q - HALO, HALO)], dst.at[pl.ds(0, HALO), mycols],
                h_ssem.at[a, 3], hl_sem.at[a], (nxt, ch),
            ).start()

    for src, dst in ((fwd, fbuf), (bwd, bbuf)):
        dst[pl.ds(HALO, Q), mycols] = src[myrows, :]

    @pl.when(ch != 0)
    def _():
        for src, dst in ((fwd, fbuf), (bwd, bbuf)):
            dst[pl.ds(0, HALO), mycols] = src[pl.ds(pl.multiple_of(ch * Q - HALO, HALO), HALO), :]

    for cp in copies:
        cp.wait()

    @pl.when(ch == 0)
    def _():
        for a, (src, dst) in enumerate(((fwd, fbuf), (bwd, bbuf))):
            remote(
                src.at[pl.ds(4 * Q - HALO, HALO)], dst.at[pl.ds(0, HALO), mycols],
                h_ssem.at[a, 3], hl_sem.at[a], (nxt, ch),
            ).wait()

    @pl.when((ch == 0) & (tm == 0))
    def _():
        zero = jnp.zeros((HALO, C), bf16)
        fbuf[pl.ds(0, HALO), :] = zero
        bbuf[pl.ds(0, HALO), :] = zero

    wide[...] = bbuf[...].astype(f32)
    u[0] = fbuf[pl.ds(HALO, Q), :]
    u[1] = wide[pl.ds(HALO - 1, Q), :].astype(bf16)

    def rest():
        s1buf[...] = u[1]
        s2buf[...] = wide[pl.ds(HALO - 2, Q), :].astype(bf16)
        wide[...] = fbuf[...].astype(f32)
        g1buf[...] = wide[pl.ds(HALO - 1, Q), :].astype(bf16)

    order_axes = ((0, 1, 2), (1, 2, 0), (2, 0, 1))

    for order in range(ORDERS):
        other = 1 - core
        po = dot_tn(u[other], u[other])
        for n, (i, j) in enumerate(TRI):
            d_send[order, pl.ds(n * BLK, BLK), :] = po[i * BLK:(i + 1) * BLK, j * BLK:(j + 1) * BLK].astype(WIRE)
        px = dot_tn(u[0, :, pl.ds(pl.multiple_of(other * 256, 256), 256)], u[1])
        for n in range(8):
            i, j = n // 4, n % 4
            d_send[order, pl.ds((10 + n) * BLK, BLK), :] = px[i * BLK:(i + 1) * BLK, j * BLK:(j + 1) * BLK].astype(WIRE)
        swap = remote(d_send.at[order], d_recv.at[order], d_ssem.at[order, 0], d_rsem.at[order, 0], partner)
        swap.start()
        po = dot_tn(u[core], u[core])
        for n, (i, j) in enumerate(TRI):
            tot[pl.ds(n * BLK, BLK), :] = po[i * BLK:(i + 1) * BLK, j * BLK:(j + 1) * BLK]
        px = dot_tn(u[0, :, pl.ds(pl.multiple_of(core * 256, 256), 256)], u[1])
        for n in range(8):
            i, j = n // 4, n % 4
            tot[pl.ds((10 + n) * BLK, BLK), :] = px[i * BLK:(i + 1) * BLK, j * BLK:(j + 1) * BLK]
        swap.wait()
        both = tot[...] + d_recv[order].astype(f32)
        tot[...] = both
        p1[order] = both.astype(WIRE)

        def sends(stage, part, pairs, axis):
            out = []
            for j in (2, 1, 3):
                src, dst = pairs(j)
                cp = remote(
                    src, dst, c_ssem.at[order, stage, part, j - 1], c_rsem.at[order, stage, part, j - 1], peer(axis, j)
                )
                cp.start()
                out.append(cp)
            return out

        st = {}
        for part, (a, b, c) in enumerate(order_axes):
            def pairs(j, part=part, a=a):
                q = lax.rem(pos[a] + j, 4)
                return (
                    p1.at[order, pl.ds(pl.multiple_of(part * PART + q * CH1, 16), CH1)],
                    r1.at[order, part, j - 1],
                )
            st[0, part] = sends(0, part, pairs, a)
        if order == 0:
            rest()
        for part, (a, b, c) in enumerate(order_axes):
            for cp in st[0, part]:
                cp.wait()
            own = tot[pl.ds(pl.multiple_of(part * PART + pos[a] * CH1, 16), CH1), :]
            total = own + r1[order, part, 0].astype(f32) + r1[order, part, 1].astype(f32) + r1[order, part, 2].astype(f32)
            acc1[part] = total
            p2[order, part] = total.astype(WIRE)

            def pairs(j, part=part, b=b):
                q = lax.rem(pos[b] + j, 4)
                return p2.at[order, part, pl.ds(pl.multiple_of(q * CH2, 16), CH2)], r2.at[order, part, j - 1]
            st[1, part] = sends(1, part, pairs, b)
        for part, (a, b, c) in enumerate(order_axes):
            for cp in st[1, part]:
                cp.wait()
            own = acc1[part, pl.ds(pl.multiple_of(pos[b] * CH2, 16), CH2), :]
            total = own + r2[order, part, 0].astype(f32) + r2[order, part, 1].astype(f32) + r2[order, part, 2].astype(f32)
            p3[order, part] = total.astype(WIRE)

            def pairs(j, part=part):
                return p3.at[order, part], r3.at[order, part, j - 1]
            st[2, part] = sends(2, part, pairs, c)
        for part, (a, b, c) in enumerate(order_axes):
            for cp in st[2, part]:
                cp.wait()
            total = (p3[order, part].astype(f32) + r3[order, part, 1].astype(f32)) + (
                r3[order, part, 0].astype(f32) + r3[order, part, 2].astype(f32)
            )
            at = pl.ds(pl.multiple_of(part * PART + pos[a] * CH1 + pos[b] * CH2, 16), CH2)
            fin[order, at, :] = total.astype(WIRE)

            def pairs(j, at=at):
                return fin.at[order, at], fin.at[order, at]
            st[3, part] = sends(3, part, pairs, b)
        for part, (a, b, c) in enumerate(order_axes):
            for cp in st[3, part]:
                cp.wait()
            at = pl.ds(pl.multiple_of(part * PART + pos[a] * CH1, 16), CH1)

            def pairs(j, at=at):
                return fin.at[order, at], fin.at[order, at]
            st[4, part] = sends(4, part, pairs, a)
        for part in range(3):
            for cp in st[4, part]:
                cp.wait()
        swap = remote(
            fin.at[order, pl.ds(10 * BLK, HALF)], fin2.at[order], d_ssem.at[order, 1], d_rsem.at[order, 1], partner
        )
        swap.start()

        square = jnp.zeros((BLK, BLK), f32)
        for n, (i, j) in enumerate(TRI):
            blk = fin[order, pl.ds(n * BLK, BLK), :].astype(f32)
            square = square + (blk * blk if i == j else 2.0 * (blk * blk))
        scale = lax.rsqrt(jnp.sum(square, keepdims=True) + 1e-06)
        for n, (i, j) in enumerate(TRI):
            blk = fin[order, pl.ds(n * BLK, BLK), :].astype(f32) * scale
            zq[pl.ds(C + i * BLK, BLK), pl.ds(j * BLK, BLK)] = blk
            if i != j:
                zq[pl.ds(C + j * BLK, BLK), pl.ds(i * BLK, BLK)] = blk.T
        swap.wait()

        @pl.when(core == 0)
        def _():
            for n in range(8):
                i, j = n // 4, n % 4
                blk = fin[order, pl.ds((10 + n) * BLK, BLK), :].astype(f32) * (-scale)
                zq[pl.ds(j * BLK, BLK), pl.ds(i * BLK, BLK)] = blk.T
                blk = fin2[order, pl.ds(n * BLK, BLK), :].astype(f32) * (-scale)
                zq[pl.ds(j * BLK, BLK), pl.ds((2 + i) * BLK, BLK)] = blk.T

        @pl.when(core == 1)
        def _():
            for n in range(8):
                i, j = n // 4, n % 4
                blk = fin[order, pl.ds((10 + n) * BLK, BLK), :].astype(f32) * (-scale)
                zq[pl.ds((2 + i) * BLK, BLK), pl.ds(j * BLK, BLK)] = blk
                blk = fin2[order, pl.ds(n * BLK, BLK), :].astype(f32) * (-scale)
                zq[pl.ds(i * BLK, BLK), pl.ds(j * BLK, BLK)] = blk

        def step(k, carry):
            v = zq[...]
            hi = v.astype(bf16)
            lo = (v - hi.astype(f32)).astype(bf16)
            prod = dot_nn(hi, hi[C:]) + (dot_nn(hi, lo[C:]) + dot_nn(lo, hi[C:]))
            zq[...] = 2.0 * v - prod
            return carry

        lax.fori_loop(0, NSTEPS - 1, step, 0)
        v = zq[...]
        hi = v.astype(bf16)
        lo = (v - hi.astype(f32)).astype(bf16)
        prod = dot_nn(hi[:C], hi[C:]) + (dot_nn(hi[:C], lo[C:]) + dot_nn(lo[:C], hi[C:]))
        amat[order, core] = (2.0 * v[:C] - prod).astype(bf16)
        swap = remote(
            amat.at[order, core], amat.at[order, core], d_ssem.at[order, 2], d_rsem.at[order, 2], partner
        )
        swap.start()
        swap.wait()
        if order == 0:
            new_f = u[0].astype(f32) + dot_nt(s1buf[...], amat[order, 1])
            new_b = s2buf[...].astype(f32) + dot_nt(g1buf[...], amat[order, 0])
            u[0] = new_f.astype(bf16)
            u[1] = new_b.astype(bf16)
        else:
            new_f = u[0].astype(f32) + dot_nt(u[1], amat[order, 1])
            new_b = u[1].astype(f32) + dot_nt(u[0], amat[order, 0])
            obuf[0] = new_f.astype(bf16)
            obuf[1] = new_b.astype(bf16)

    copies = []
    for j in (2, 1, 3):
        t = lax.rem(ch + j, 4)
        for a, dst in enumerate((out_f, out_b)):
            cp = remote(
                obuf.at[a, :, pl.ds(pl.multiple_of(t * W, W), W)], dst.at[myrows],
                o_ssem.at[a, j - 1], o_rsem.at[a, j - 1], (tm, t),
            )
            cp.start()
            copies.append(cp)
    for a, dst in enumerate((out_f, out_b)):
        dst[myrows, :] = obuf[a, :, mycols]
    for cp in copies:
        cp.wait()


def local(fwd_in, bwd_in):
    vmem = pl.BlockSpec(memory_space=pltpu.VMEM)
    rows = fwd_in.shape[0]
    dma = pltpu.SemaphoreType.DMA
    return pl.pallas_call(
        kernel,
        out_shape=(jax.ShapeDtypeStruct((rows, W), bf16), jax.ShapeDtypeStruct((rows, W), bf16)),
        in_specs=[vmem, vmem],
        out_specs=(vmem, vmem),
        scratch_shapes=[
            pltpu.VMEM((Q + HALO, C), bf16),
            pltpu.VMEM((Q + HALO, C), bf16),
            pltpu.VMEM((Q + HALO, C), f32),
            pltpu.VMEM((2, Q, C), bf16),
            pltpu.VMEM((Q, C), bf16),
            pltpu.VMEM((Q, C), bf16),
            pltpu.VMEM((Q, C), bf16),
            pltpu.VMEM((ORDERS, ROWS, BLK), WIRE),
            pltpu.VMEM((ORDERS, ROWS, BLK), WIRE),
            pltpu.VMEM((ROWS, BLK), f32),
            pltpu.VMEM((ORDERS, ROWS, BLK), WIRE),
            pltpu.VMEM((ORDERS, 3, 3, CH1, BLK), WIRE),
            pltpu.VMEM((3, CH1, BLK), f32),
            pltpu.VMEM((ORDERS, 3, CH1, BLK), WIRE),
            pltpu.VMEM((ORDERS, 3, 3, CH2, BLK), WIRE),
            pltpu.VMEM((3, CH2, BLK), f32),
            pltpu.VMEM((ORDERS, 3, CH2, BLK), WIRE),
            pltpu.VMEM((ORDERS, 3, 3, CH2, BLK), WIRE),
            pltpu.VMEM((ORDERS, ROWS, BLK), WIRE),
            pltpu.VMEM((ORDERS, HALF, BLK), WIRE),
            pltpu.VMEM((2 * C, C), f32),
            pltpu.VMEM((ORDERS, 2, C, C), bf16),
            pltpu.VMEM((2, Q, C), bf16),
            dma((2, 3)), dma((2, 3)), dma((2, 4)), dma((2, 3)), dma((2,)),
            dma((ORDERS, 3)), dma((ORDERS, 3)),
            dma((ORDERS, 5, 3, 3)), dma((ORDERS, 5, 3, 3)),
            dma((2, 3)), dma((2, 3)),
        ],
        compiler_params=pltpu.CompilerParams(
            collective_id=0, has_side_effects=True, vmem_limit_bytes=48 * 1024 * 1024
        ),
        name="lattice",
    )(fwd_in, bwd_in)


def solution(mesh):
    in_specs = (P("tm", "chan"), P("tm", "chan"))
    out_specs = (P("tm", "chan"), P("tm", "chan"))
    return jax.shard_map(local, mesh=mesh, in_specs=in_specs, out_specs=out_specs, check_vma=False)
```

```python
import jax
import jax.numpy as jnp
from jax import lax
from jax.experimental import pallas as pl
from jax.experimental.pallas import tpu as pltpu
from jax.sharding import PartitionSpec as P

ORDERS = 2
NSTEPS = 6
C = 512
W = 128
Q = 512
HALO = 16
BLK = 128
TRI = [(i, j) for i in range(4) for j in range(i, 4)]
ROWS = 18 * BLK
PART = ROWS // 3
CH1 = PART // 4
CH2 = CH1 // 4
HALF = 8 * BLK
MESH = pl.DeviceIdType.MESH
f32 = jnp.float32
bf16 = jnp.bfloat16
NEAR = bf16
FIRST = bf16


def dot_tn(a, b):
    return lax.dot_general(a, b, (((0,), (0,)), ((), ())), preferred_element_type=f32)


def dot_nt(a, b):
    return lax.dot_general(a, b, (((1,), (1,)), ((), ())), preferred_element_type=f32)


def dot_nn(a, b):
    return lax.dot_general(a, b, (((1,), (0,)), ((), ())), preferred_element_type=f32)


def kernel(
    fwd, bwd, out_f, out_b,
    ff, bb, hf, hb, wide, u, s1buf, s2buf, g1buf, nf, ns,
    d_send, d_recv, tot, p1, r1, p2, r2, p3, r3, fin, fin2,
    zmat, emat, amat,
    l_sem, x_ssem, x_rsem, h_ssem, h_rsem, hl_sem, g_ssem, g_rsem, f_ssem, f_rsem,
    d_ssem, d_rsem, c_ssem, c_rsem,
):
    tm = lax.axis_index("tm")
    ch = lax.axis_index("chan")
    y_hi, zx = lax.div(tm, 16), lax.rem(tm, 16)
    z, x = lax.div(zx, 4), lax.rem(zx, 4)
    y_lo, core = lax.div(ch, 2), lax.rem(ch, 2)
    y = y_hi * 2 + y_lo
    partner = (tm, y_lo * 2 + 1 - core)

    def peer(axis, j):
        if axis == 0:
            return (tm - x + lax.rem(x + j, 4), ch)
        if axis == 1:
            ny = lax.rem(y + j, 4)
            return (lax.div(ny, 2) * 16 + zx, lax.rem(ny, 2) * 2 + core)
        return (y_hi * 16 + lax.rem(z + j, 4) * 4 + x, ch)

    pos = (x, y, z)
    nxt = lax.rem(tm + 1, 32)
    prv = lax.rem(tm + 31, 32)

    barrier = pltpu.get_barrier_semaphore()
    for j in (1, 2, 3):
        pl.semaphore_signal(barrier, inc=1, device_id=(tm, lax.rem(ch + j, 4)), device_id_type=MESH)
        for axis in range(3):
            pl.semaphore_signal(barrier, inc=1, device_id=peer(axis, j), device_id_type=MESH)
    for k in range(4):
        pl.semaphore_signal(barrier, inc=1, device_id=(prv, k), device_id_type=MESH)

    mycols = pl.ds(pl.multiple_of(ch * W, W), W)
    whole = pl.ds(HALO, 4 * Q)
    loads = []
    for a, (src, dst) in enumerate(((fwd, ff), (bwd, bb))):
        cp = pltpu.make_async_copy(src, dst.at[whole, mycols], l_sem.at[a])
        cp.start()
        loads.append(cp)
    pl.semaphore_wait(barrier, 16)
    for cp in loads:
        cp.wait()

    def remote(src, dst, ssem, rsem, dev):
        return pltpu.make_async_remote_copy(
            src_ref=src, dst_ref=dst, send_sem=ssem, recv_sem=rsem, device_id=dev, device_id_type=MESH
        )

    def quarter(t):
        return pl.ds(pl.multiple_of(HALO + t * Q, HALO), Q)

    arrays = ((ff, hf), (bb, hb))
    far = (1 - y_lo) * 2
    copies, late = [], []
    for a, (buf, ahead) in enumerate(arrays):
        for j in (1, 2, 3):
            t = lax.rem(ch + j, 4)
            k = lax.rem(t + 3, 4)
            copies.append(remote(
                buf.at[pl.ds(pl.multiple_of((k + 1) * Q, HALO), HALO), mycols], ahead.at[:, mycols],
                h_ssem.at[a, j - 1], h_rsem.at[a, j - 1], (jnp.where(t == 0, nxt, tm), t),
            ))
    for k in range(2):
        t = far + lax.rem(core + k, 2)
        for a, (buf, ahead) in enumerate(arrays):
            copies.append(remote(
                buf.at[quarter(t), mycols], buf.at[quarter(t), mycols],
                x_ssem.at[a, k], x_rsem.at[a, k], (tm, t),
            ))
    for a, (buf, ahead) in enumerate(arrays):
        copies.append(remote(
            buf.at[whole, mycols], buf.at[whole, mycols], x_ssem.at[a, 2], x_rsem.at[a, 2], partner
        ))
    for a, (buf, ahead) in enumerate(arrays):
        for t in range(4):
            late.append(remote(
                buf.at[pl.ds(4 * Q, HALO), mycols], buf.at[pl.ds(0, HALO), mycols],
                g_ssem.at[a, t], g_rsem.at[a, lax.rem(ch - t + 4, 4)], (nxt, t),
            ))
    for cp in copies + late:
        cp.start()

    def own_ahead(a):
        buf, ahead = arrays[a]
        return remote(
            buf.at[pl.ds(4 * Q, HALO), mycols], ahead.at[:, mycols], h_ssem.at[a, 3], hl_sem.at[a], (nxt, ch)
        )

    @pl.when(ch == 0)
    def _():
        for a in range(2):
            own_ahead(a).start()

    @pl.when(ch != 0)
    def _():
        for buf, ahead in arrays:
            ahead[:, mycols] = buf[pl.ds(pl.multiple_of(ch * Q, HALO), HALO), mycols]

    for cp in copies:
        cp.wait()

    @pl.when(ch == 0)
    def _():
        for a in range(2):
            own_ahead(a).wait()

    @pl.when((ch == 0) & (tm == 0))
    def _():
        hf[...] = jnp.zeros_like(hf)
        hb[...] = jnp.zeros_like(hb)

    def widen(buf, t, ahead):
        if ahead is None:
            wide[...] = buf[pl.ds(pl.multiple_of(t * Q, HALO), Q + HALO), :].astype(f32)
        else:
            wide[pl.ds(0, HALO), :] = ahead[...].astype(f32)
            wide[pl.ds(HALO, Q), :] = buf[quarter(t), :].astype(f32)

    def behind(by):
        return wide[pl.ds(HALO - by, Q), :]

    widen(bb, ch, hb)
    u[0] = ff[quarter(ch), :]
    u[1] = behind(1).astype(bf16)

    def share_quarter():
        out = []
        cols = pl.ds(pl.multiple_of(far * W, 2 * W), 2 * W)
        for a, (buf, ahead) in enumerate(arrays):
            cp = remote(
                buf.at[quarter(ch), cols], buf.at[quarter(ch), cols], f_ssem.at[a, 0], f_rsem.at[a, 0], partner
            )
            cp.start()
            out.append(cp)
        return out

    def send_half():
        out = []
        rows = pl.ds(pl.multiple_of(HALO + y_lo * 2 * Q, HALO), 2 * Q)
        for a, (buf, ahead) in enumerate(arrays):
            cp = remote(
                buf.at[rows, mycols], buf.at[rows, mycols], f_ssem.at[a, 1], f_rsem.at[a, 1], (tm, far + core)
            )
            cp.start()
            out.append(cp)
        return out

    def share_half():
        out = []
        rows = pl.ds(pl.multiple_of(HALO + far * Q, HALO), 2 * Q)
        cols = pl.ds(pl.multiple_of((far + core) * W, W), W)
        for a, (buf, ahead) in enumerate(arrays):
            cp = remote(
                buf.at[rows, cols], buf.at[rows, cols], f_ssem.at[a, 2], f_rsem.at[a, 2], partner
            )
            cp.start()
            out.append(cp)
        return out

    def rest():
        s1buf[...] = u[1]
        s2buf[...] = behind(2).astype(bf16)
        widen(ff, ch, hf)
        g1buf[...] = behind(1).astype(bf16)
        for cp in late:
            cp.wait()

        @pl.when(tm == 0)
        def _():
            ff[pl.ds(0, HALO), :] = jnp.zeros((HALO, C), bf16)
            bb[pl.ds(0, HALO), :] = jnp.zeros((HALO, C), bf16)

    def advance(t):
        rows = pl.ds(pl.multiple_of(t * Q, Q), Q)
        widen(bb, t, None)
        nf[rows, :] = (ff[quarter(t), :].astype(f32) + dot_nt(behind(1).astype(bf16), amat[0, 1])).astype(bf16)
        keep = behind(2)
        widen(ff, t, None)
        ns[rows, :] = (keep + dot_nt(behind(1).astype(bf16), amat[0, 0])).astype(bf16)

    eye = lax.broadcasted_iota(jnp.int32, (BLK, BLK), 0) == lax.broadcasted_iota(jnp.int32, (BLK, BLK), 1)

    def diagonal(m):
        blocks = [jnp.where(eye, m[i * BLK:(i + 1) * BLK, i * BLK:(i + 1) * BLK], 0.0) for i in range(4)]
        return (
            jnp.concatenate([jnp.sum(b, axis=0, keepdims=True) for b in blocks], axis=1),
            jnp.concatenate([jnp.sum(b, axis=1, keepdims=True) for b in blocks], axis=0),
        )

    order_axes = ((0, 1, 2), (1, 2, 0), (2, 0, 1))

    for order in range(ORDERS):
        other = 1 - core
        po = dot_tn(u[other], u[other])
        for n, (i, j) in enumerate(TRI):
            d_send[order, pl.ds(n * BLK, BLK), :] = po[i * BLK:(i + 1) * BLK, j * BLK:(j + 1) * BLK].astype(NEAR)
        px = dot_tn(u[0, :, pl.ds(pl.multiple_of(other * 256, 256), 256)], u[1])
        for n in range(8):
            i, j = n // 4, n % 4
            d_send[order, pl.ds((10 + n) * BLK, BLK), :] = px[i * BLK:(i + 1) * BLK, j * BLK:(j + 1) * BLK].astype(NEAR)
        swap = remote(d_send.at[order], d_recv.at[order], d_ssem.at[order, 0], d_rsem.at[order, 0], partner)
        swap.start()
        po = dot_tn(u[core], u[core])
        for n, (i, j) in enumerate(TRI):
            tot[pl.ds(n * BLK, BLK), :] = po[i * BLK:(i + 1) * BLK, j * BLK:(j + 1) * BLK]
        px = dot_tn(u[0, :, pl.ds(pl.multiple_of(core * 256, 256), 256)], u[1])
        for n in range(8):
            i, j = n // 4, n % 4
            tot[pl.ds((10 + n) * BLK, BLK), :] = px[i * BLK:(i + 1) * BLK, j * BLK:(j + 1) * BLK]
        swap.wait()
        both = tot[...] + d_recv[order].astype(f32)
        tot[...] = both
        p1[order] = both.astype(FIRST)

        def sends(stage, part, pairs, axis):
            out = []
            for j in (2, 1, 3):
                src, dst = pairs(j)
                cp = remote(
                    src, dst, c_ssem.at[order, stage, part, j - 1], c_rsem.at[order, stage, part, j - 1], peer(axis, j)
                )
                cp.start()
                out.append(cp)
            return out

        st = {}
        for part, (a, b, c) in enumerate(order_axes):
            def pairs(j, part=part, a=a):
                q = lax.rem(pos[a] + j, 4)
                return (
                    p1.at[order, pl.ds(pl.multiple_of(part * PART + q * CH1, 16), CH1)],
                    r1.at[order, part, j - 1],
                )
            st[0, part] = sends(0, part, pairs, a)
        if order == 0:
            shares = share_quarter()
            rest()
        else:
            for cp in shares:
                cp.wait()
            shares = share_half()
            rows = pl.ds(pl.multiple_of(ch * Q, Q), Q)
            nf[rows, :] = u[0]
            ns[rows, :] = u[1]
            for cp in shares:
                cp.wait()
            advance(lax.rem(ch + 1, 4))
        for part, (a, b, c) in enumerate(order_axes):
            for cp in st[0, part]:
                cp.wait()
            own = tot[pl.ds(pl.multiple_of(part * PART + pos[a] * CH1, 16), CH1), :]
            total = own + r1[order, part, 0].astype(f32) + r1[order, part, 1].astype(f32) + r1[order, part, 2].astype(f32)
            p2[order, part] = total

            def pairs(j, part=part, b=b):
                q = lax.rem(pos[b] + j, 4)
                return p2.at[order, part, pl.ds(pl.multiple_of(q * CH2, 16), CH2)], r2.at[order, part, j - 1]
            st[1, part] = sends(1, part, pairs, b)
        if order == 1:
            advance(lax.rem(ch + 2, 4))
        for part, (a, b, c) in enumerate(order_axes):
            for cp in st[1, part]:
                cp.wait()
            own = p2[order, part, pl.ds(pl.multiple_of(pos[b] * CH2, 16), CH2), :]
            total = own + r2[order, part, 0] + r2[order, part, 1] + r2[order, part, 2]
            p3[order, part] = total

            def pairs(j, part=part):
                return p3.at[order, part], r3.at[order, part, j - 1]
            st[2, part] = sends(2, part, pairs, c)
        if order == 1:
            advance(lax.rem(ch + 3, 4))
        for part, (a, b, c) in enumerate(order_axes):
            for cp in st[2, part]:
                cp.wait()
            total = (p3[order, part] + r3[order, part, 1]) + (r3[order, part, 0] + r3[order, part, 2])
            at = pl.ds(pl.multiple_of(part * PART + pos[a] * CH1 + pos[b] * CH2, 16), CH2)
            fin[order, at, :] = total

            def pairs(j, at=at):
                return fin.at[order, at], fin.at[order, at]
            st[3, part] = sends(3, part, pairs, b)
        for part, (a, b, c) in enumerate(order_axes):
            for cp in st[3, part]:
                cp.wait()
            at = pl.ds(pl.multiple_of(part * PART + pos[a] * CH1, 16), CH1)

            def pairs(j, at=at):
                return fin.at[order, at], fin.at[order, at]
            st[4, part] = sends(4, part, pairs, a)
        for part in range(3):
            for cp in st[4, part]:
                cp.wait()
        if order == 0:
            for cp in shares:
                cp.wait()
            shares = send_half()
        swap = remote(
            fin.at[order, pl.ds(10 * BLK, HALF)], fin2.at[order], d_ssem.at[order, 1], d_rsem.at[order, 1], partner
        )
        swap.start()

        square = jnp.zeros((BLK, BLK), f32)
        for n, (i, j) in enumerate(TRI):
            blk = fin[order, pl.ds(n * BLK, BLK), :]
            square = square + (blk * blk if i == j else 2.0 * (blk * blk))
        scale = lax.rsqrt(jnp.sum(square, keepdims=True) + 1e-06)
        rows_d, cols_d = [], []
        for n, (i, j) in enumerate(TRI):
            blk = fin[order, pl.ds(n * BLK, BLK), :] * scale
            if i == j:
                only = jnp.where(eye, blk, 0.0)
                rows_d.append(jnp.sum(only, axis=0, keepdims=True))
                cols_d.append(jnp.sum(only, axis=1, keepdims=True))
                emat[pl.ds(i * BLK, BLK), pl.ds(j * BLK, BLK)] = jnp.where(eye, 0.0, blk)
            else:
                emat[pl.ds(i * BLK, BLK), pl.ds(j * BLK, BLK)] = blk
                emat[pl.ds(j * BLK, BLK), pl.ds(i * BLK, BLK)] = blk.T
        swap.wait()

        @pl.when(core == 0)
        def _():
            for n in range(8):
                i, j = n // 4, n % 4
                blk = fin[order, pl.ds((10 + n) * BLK, BLK), :] * (-scale)
                zmat[pl.ds(j * BLK, BLK), pl.ds(i * BLK, BLK)] = blk.T
                blk = fin2[order, pl.ds(n * BLK, BLK), :] * (-scale)
                zmat[pl.ds(j * BLK, BLK), pl.ds((2 + i) * BLK, BLK)] = blk.T

        @pl.when(core == 1)
        def _():
            for n in range(8):
                i, j = n // 4, n % 4
                blk = fin[order, pl.ds((10 + n) * BLK, BLK), :] * (-scale)
                zmat[pl.ds((2 + i) * BLK, BLK), pl.ds(j * BLK, BLK)] = blk
                blk = fin2[order, pl.ds(n * BLK, BLK), :] * (-scale)
                zmat[pl.ds(i * BLK, BLK), pl.ds(j * BLK, BLK)] = blk

        zrows = pl.ds(0, C) if order == 0 else pl.ds(pl.multiple_of(y_lo * 2 * W, 2 * W), 2 * W)

        def step(k, carry):
            dr, dc = carry
            e = emat[...]
            eb = e.astype(bf16)
            te = dot_nn(eb, eb)
            tr, tc = diagonal(te)
            zv = zmat[zrows, :]
            zmat[zrows, :] = zv * (2.0 - dr) - dot_nn(zv.astype(bf16), eb)
            emat[...] = e * ((2.0 - dc) - dr) - te
            for i in range(4):
                at = pl.ds(i * BLK, BLK)
                emat[at, at] = jnp.where(eye, 0.0, emat[at, at])
            return 2.0 * dr - dr * dr - tr, 2.0 * dc - dc * dc - tc

        dr, dc = lax.fori_loop(
            0, NSTEPS - 1, step, (jnp.concatenate(rows_d, axis=1), jnp.concatenate(cols_d, axis=0))
        )
        zv = zmat[zrows, :]
        amat[order, core, zrows, :] = (
            zv * (2.0 - dr) - dot_nn(zv.astype(bf16), emat[...].astype(bf16))
        ).astype(bf16)
        if order == 0:
            part_rows = pl.ds(0, C)
        else:
            part_rows = pl.ds(pl.multiple_of((y_lo * 2 + 1 - core) * W, W), W)
        swap = remote(
            amat.at[order, core, part_rows], amat.at[order, core, part_rows],
            d_ssem.at[order, 2], d_rsem.at[order, 2], partner,
        )
        swap.start()
        swap.wait()
        if order == 0:
            new_f = u[0].astype(f32) + dot_nt(s1buf[...], amat[order, 1])
            new_b = s2buf[...].astype(f32) + dot_nt(g1buf[...], amat[order, 0])
            u[0] = new_f.astype(bf16)
            u[1] = new_b.astype(bf16)

    for t in range(4):
        rows = pl.ds(t * Q, Q)
        out_f[rows, :] = (nf[rows, mycols].astype(f32) + dot_nt(ns[rows, :], amat[1, 1, mycols, :])).astype(bf16)
        out_b[rows, :] = (ns[rows, mycols].astype(f32) + dot_nt(nf[rows, :], amat[1, 0, mycols, :])).astype(bf16)


def local(fwd_in, bwd_in):
    vmem = pl.BlockSpec(memory_space=pltpu.VMEM)
    hbm = pl.BlockSpec(memory_space=pltpu.HBM)
    rows = fwd_in.shape[0]
    dma = pltpu.SemaphoreType.DMA
    return pl.pallas_call(
        kernel,
        out_shape=(jax.ShapeDtypeStruct((rows, W), bf16), jax.ShapeDtypeStruct((rows, W), bf16)),
        in_specs=[hbm, hbm],
        out_specs=(vmem, vmem),
        scratch_shapes=[
            pltpu.VMEM((HALO + rows, C), bf16),
            pltpu.VMEM((HALO + rows, C), bf16),
            pltpu.VMEM((HALO, C), bf16),
            pltpu.VMEM((HALO, C), bf16),
            pltpu.VMEM((Q + HALO, C), f32),
            pltpu.VMEM((2, Q, C), bf16),
            pltpu.VMEM((Q, C), bf16),
            pltpu.VMEM((Q, C), bf16),
            pltpu.VMEM((Q, C), bf16),
            pltpu.VMEM((rows, C), bf16),
            pltpu.VMEM((rows, C), bf16),
            pltpu.VMEM((ORDERS, ROWS, BLK), NEAR),
            pltpu.VMEM((ORDERS, ROWS, BLK), NEAR),
            pltpu.VMEM((ROWS, BLK), f32),
            pltpu.VMEM((ORDERS, ROWS, BLK), FIRST),
            pltpu.VMEM((ORDERS, 3, 3, CH1, BLK), FIRST),
            pltpu.VMEM((ORDERS, 3, CH1, BLK), f32),
            pltpu.VMEM((ORDERS, 3, 3, CH2, BLK), f32),
            pltpu.VMEM((ORDERS, 3, CH2, BLK), f32),
            pltpu.VMEM((ORDERS, 3, 3, CH2, BLK), f32),
            pltpu.VMEM((ORDERS, ROWS, BLK), f32),
            pltpu.VMEM((ORDERS, HALF, BLK), f32),
            pltpu.VMEM((C, C), f32),
            pltpu.VMEM((C, C), f32),
            pltpu.VMEM((ORDERS, 2, C, C), bf16),
            dma((2,)), dma((2, 3)), dma((2, 3)), dma((2, 4)), dma((2, 3)), dma((2,)),
            dma((2, 4)), dma((2, 4)), dma((2, 3)), dma((2, 3)),
            dma((ORDERS, 3)), dma((ORDERS, 3)),
            dma((ORDERS, 5, 3, 3)), dma((ORDERS, 5, 3, 3)),
        ],
        compiler_params=pltpu.CompilerParams(
            collective_id=0, has_side_effects=True, vmem_limit_bytes=56 * 1024 * 1024
        ),
        name="lattice",
    )(fwd_in, bwd_in)


def solution(mesh):
    in_specs = (P("tm", "chan"), P("tm", "chan"))
    out_specs = (P("tm", "chan"), P("tm", "chan"))
    return jax.shard_map(local, mesh=mesh, in_specs=in_specs, out_specs=out_specs, check_vma=False)
```

```python
import jax
import jax.numpy as jnp
from jax import lax
from jax.experimental import pallas as pl
from jax.experimental.pallas import tpu as pltpu
from jax.sharding import PartitionSpec as P

ORDERS = 2
NSTEPS = 6
C = 512
W = 128
Q = 512
HALO = 16
BLK = 128
TRI = [(i, j) for i in range(4) for j in range(i, 4)]
GROUPS = ((0, 1536, 512, 128, 32), (1536, 1152, 384, 96, 24))
ROWS = 2688
HALF = 8 * BLK
MESH = pl.DeviceIdType.MESH
f32 = jnp.float32
bf16 = jnp.bfloat16
NEAR = bf16
FIRST = bf16


def dot_tn(a, b):
    return lax.dot_general(a, b, (((0,), (0,)), ((), ())), preferred_element_type=f32)


def dot_nt(a, b):
    return lax.dot_general(a, b, (((1,), (1,)), ((), ())), preferred_element_type=f32)


def dot_nn(a, b):
    return lax.dot_general(a, b, (((1,), (0,)), ((), ())), preferred_element_type=f32)


def kernel(
    fwd, bwd, out_f, out_b,
    ff, bb, hf, hb, wide, u, s1buf, s2buf, g1buf, nf, ns,
    d_send, d_recv, tot, p1, r1a, r1b, p2a, p2b, r2a, r2b, p3a, p3b, r3a, r3b, fin_a, fin_b, far_half,
    zmat, emat, xmat, amat,
    l_sem, x_ssem, x_rsem, h_ssem, h_rsem, hl_sem, g_ssem, g_rsem, f_ssem, f_rsem,
    d_ssem, d_rsem, c_ssem, c_rsem,
):
    r1, p2, r2, p3, r3, fin = (r1a, r1b), (p2a, p2b), (r2a, r2b), (p3a, p3b), (r3a, r3b), (fin_a, fin_b)
    tm = lax.axis_index("tm")
    ch = lax.axis_index("chan")
    y_hi, zx = lax.div(tm, 16), lax.rem(tm, 16)
    z, x = lax.div(zx, 4), lax.rem(zx, 4)
    y_lo, core = lax.div(ch, 2), lax.rem(ch, 2)
    y = y_hi * 2 + y_lo
    partner = (tm, y_lo * 2 + 1 - core)

    def peer(axis, j):
        if axis == 0:
            return (tm - x + lax.rem(x + j, 4), ch)
        if axis == 1:
            ny = lax.rem(y + j, 4)
            return (lax.div(ny, 2) * 16 + zx, lax.rem(ny, 2) * 2 + core)
        return (y_hi * 16 + lax.rem(z + j, 4) * 4 + x, ch)

    pos = (x, y, z)
    nxt = lax.rem(tm + 1, 32)
    prv = lax.rem(tm + 31, 32)

    barrier = pltpu.get_barrier_semaphore()
    for j in (1, 2, 3):
        pl.semaphore_signal(barrier, inc=1, device_id=(tm, lax.rem(ch + j, 4)), device_id_type=MESH)
        for axis in range(3):
            pl.semaphore_signal(barrier, inc=1, device_id=peer(axis, j), device_id_type=MESH)
    for k in range(4):
        pl.semaphore_signal(barrier, inc=1, device_id=(prv, k), device_id_type=MESH)

    mycols = pl.ds(pl.multiple_of(ch * W, W), W)
    whole = pl.ds(HALO, 4 * Q)
    loads = []
    for a, (src, dst) in enumerate(((fwd, ff), (bwd, bb))):
        cp = pltpu.make_async_copy(src, dst.at[whole, mycols], l_sem.at[a])
        cp.start()
        loads.append(cp)
    pl.semaphore_wait(barrier, 16)
    for cp in loads:
        cp.wait()

    def remote(src, dst, ssem, rsem, dev):
        return pltpu.make_async_remote_copy(
            src_ref=src, dst_ref=dst, send_sem=ssem, recv_sem=rsem, device_id=dev, device_id_type=MESH
        )

    def quarter(t):
        return pl.ds(pl.multiple_of(HALO + t * Q, HALO), Q)

    arrays = ((ff, hf), (bb, hb))
    far = (1 - y_lo) * 2
    copies, late = [], []
    for a, (buf, ahead) in enumerate(arrays):
        for j in (1, 2, 3):
            t = lax.rem(ch + j, 4)
            k = lax.rem(t + 3, 4)
            copies.append(remote(
                buf.at[pl.ds(pl.multiple_of((k + 1) * Q, HALO), HALO), mycols], ahead.at[:, mycols],
                h_ssem.at[a, j - 1], h_rsem.at[a, j - 1], (jnp.where(t == 0, nxt, tm), t),
            ))
    for k in range(2):
        t = far + lax.rem(core + k, 2)
        for a, (buf, ahead) in enumerate(arrays):
            copies.append(remote(
                buf.at[quarter(t), mycols], buf.at[quarter(t), mycols],
                x_ssem.at[a, k], x_rsem.at[a, k], (tm, t),
            ))
    for a, (buf, ahead) in enumerate(arrays):
        copies.append(remote(
            buf.at[whole, mycols], buf.at[whole, mycols], x_ssem.at[a, 2], x_rsem.at[a, 2], partner
        ))
    for a, (buf, ahead) in enumerate(arrays):
        for t in range(4):
            late.append(remote(
                buf.at[pl.ds(4 * Q, HALO), mycols], buf.at[pl.ds(0, HALO), mycols],
                g_ssem.at[a, t], g_rsem.at[a, lax.rem(ch - t + 4, 4)], (nxt, t),
            ))
    for cp in copies + late:
        cp.start()

    def own_ahead(a):
        buf, ahead = arrays[a]
        return remote(
            buf.at[pl.ds(4 * Q, HALO), mycols], ahead.at[:, mycols], h_ssem.at[a, 3], hl_sem.at[a], (nxt, ch)
        )

    @pl.when(ch == 0)
    def _():
        for a in range(2):
            own_ahead(a).start()

    @pl.when(ch != 0)
    def _():
        for buf, ahead in arrays:
            ahead[:, mycols] = buf[pl.ds(pl.multiple_of(ch * Q, HALO), HALO), mycols]

    for cp in copies:
        cp.wait()

    @pl.when(ch == 0)
    def _():
        for a in range(2):
            own_ahead(a).wait()

    @pl.when((ch == 0) & (tm == 0))
    def _():
        hf[...] = jnp.zeros_like(hf)
        hb[...] = jnp.zeros_like(hb)

    def widen(buf, t, ahead):
        if ahead is None:
            wide[...] = buf[pl.ds(pl.multiple_of(t * Q, HALO), Q + HALO), :].astype(f32)
        else:
            wide[pl.ds(0, HALO), :] = ahead[...].astype(f32)
            wide[pl.ds(HALO, Q), :] = buf[quarter(t), :].astype(f32)

    def behind(by):
        return wide[pl.ds(HALO - by, Q), :]

    widen(bb, ch, hb)
    u[0] = ff[quarter(ch), :]
    u[1] = behind(1).astype(bf16)

    def share_quarter():
        out = []
        cols = pl.ds(pl.multiple_of(far * W, 2 * W), 2 * W)
        for a, (buf, ahead) in enumerate(arrays):
            cp = remote(
                buf.at[quarter(ch), cols], buf.at[quarter(ch), cols], f_ssem.at[a, 0], f_rsem.at[a, 0], partner
            )
            cp.start()
            out.append(cp)
        return out

    def send_half():
        out = []
        rows = pl.ds(pl.multiple_of(HALO + y_lo * 2 * Q, HALO), 2 * Q)
        for a, (buf, ahead) in enumerate(arrays):
            cp = remote(
                buf.at[rows, mycols], buf.at[rows, mycols], f_ssem.at[a, 1], f_rsem.at[a, 1], (tm, far + core)
            )
            cp.start()
            out.append(cp)
        return out

    def share_half():
        out = []
        rows = pl.ds(pl.multiple_of(HALO + far * Q, HALO), 2 * Q)
        cols = pl.ds(pl.multiple_of((far + core) * W, W), W)
        for a, (buf, ahead) in enumerate(arrays):
            cp = remote(
                buf.at[rows, cols], buf.at[rows, cols], f_ssem.at[a, 2], f_rsem.at[a, 2], partner
            )
            cp.start()
            out.append(cp)
        return out

    def rest():
        s1buf[...] = u[1]
        s2buf[...] = behind(2).astype(bf16)
        widen(ff, ch, hf)
        g1buf[...] = behind(1).astype(bf16)
        for cp in late:
            cp.wait()

        @pl.when(tm == 0)
        def _():
            ff[pl.ds(0, HALO), :] = jnp.zeros((HALO, C), bf16)
            bb[pl.ds(0, HALO), :] = jnp.zeros((HALO, C), bf16)

    def advance(t):
        rows = pl.ds(pl.multiple_of(t * Q, Q), Q)
        widen(bb, t, None)
        nf[rows, :] = (ff[quarter(t), :].astype(f32) + dot_nt(behind(1).astype(bf16), amat[0, 1])).astype(bf16)
        keep = behind(2)
        widen(ff, t, None)
        ns[rows, :] = (keep + dot_nt(behind(1).astype(bf16), amat[0, 0])).astype(bf16)

    eye = lax.broadcasted_iota(jnp.int32, (BLK, BLK), 0) == lax.broadcasted_iota(jnp.int32, (BLK, BLK), 1)

    def diagonal(m):
        blocks = [jnp.where(eye, m[i * BLK:(i + 1) * BLK, i * BLK:(i + 1) * BLK], 0.0) for i in range(4)]
        return (
            jnp.concatenate([jnp.sum(b, axis=0, keepdims=True) for b in blocks], axis=1),
            jnp.concatenate([jnp.sum(b, axis=1, keepdims=True) for b in blocks], axis=0),
        )

    order_axes = ((0, 1, 2), (1, 2, 0), (2, 0, 1))
    other = 1 - core

    def half(k):
        return u[0, :, pl.ds(pl.multiple_of(k * 256, 256), 256)]

    def put_tri(dst, m):
        for n, (i, j) in enumerate(TRI):
            dst[pl.ds(n * BLK, BLK), :] = m[i * BLK:(i + 1) * BLK, j * BLK:(j + 1) * BLK].astype(dst.dtype)

    def put_cross(dst, m):
        for n in range(8):
            i, j = n // 4, n % 4
            dst[pl.ds(GROUPS[1][0] + n * BLK, BLK), :] = m[
                i * BLK:(i + 1) * BLK, j * BLK:(j + 1) * BLK
            ].astype(dst.dtype)

    lane = lax.broadcasted_iota(jnp.int32, (BLK, BLK), 1)
    row = lax.broadcasted_iota(jnp.int32, (BLK, BLK), 0)
    kept = ((lane > row) & ~((row == 0) & (lane == BLK - 1))) | ((row == BLK - 1) & (lane == 0))

    for order in range(ORDERS):
        swapped = pl.ds(0, 10 * BLK), pl.ds(GROUPS[1][0], HALF)

        def swap_part(k):
            return remote(
                d_send.at[order, swapped[k]], d_recv.at[order, swapped[k]],
                d_ssem.at[order, k], d_rsem.at[order, k], partner,
            )

        put_tri(d_send.at[order], dot_tn(u[other], u[other]))
        swap_part(0).start()
        put_cross(d_send.at[order], dot_tn(half(other), u[1]))
        swap_part(1).start()
        put_tri(tot, dot_tn(u[core], u[core]))

        def sends(g, stage, part, pairs, axis):
            out = []
            for j in (2, 1, 3):
                src, dst = pairs(j)
                cp = remote(
                    src, dst, c_ssem.at[order, g, stage, part, j - 1], c_rsem.at[order, g, stage, part, j - 1],
                    peer(axis, j),
                )
                cp.start()
                out.append(cp)
            return out

        st = {}

        def done(g, stage, part):
            for cp in st[g, stage, part]:
                cp.wait()

        def stage0(g):
            base, rows, size, c1, c2 = GROUPS[g]
            swap_part(g).wait()
            at = swapped[g]
            both = tot[at, :] + d_recv[order, at, :].astype(f32)
            tot[at, :] = both
            p1[order, at, :] = both.astype(FIRST)
            for part, (a, b, c) in enumerate(order_axes):
                def pairs(j):
                    q = lax.rem(pos[a] + j, 4)
                    return (
                        p1.at[order, pl.ds(pl.multiple_of(base + part * size + q * c1, 16), c1)],
                        r1[g].at[order, part, j - 1],
                    )
                st[g, 0, part] = sends(g, 0, part, pairs, a)

        def stage1(g):
            base, rows, size, c1, c2 = GROUPS[g]
            for part, (a, b, c) in enumerate(order_axes):
                done(g, 0, part)
                r = r1[g]
                own = tot[pl.ds(pl.multiple_of(base + part * size + pos[a] * c1, 16), c1), :]
                p2[g][order, part] = own + r[order, part, 0].astype(f32) + r[order, part, 1].astype(f32) + r[
                    order, part, 2
                ].astype(f32)

                def pairs(j):
                    q = lax.rem(pos[b] + j, 4)
                    return p2[g].at[order, part, pl.ds(pl.multiple_of(q * c2, 8), c2)], r2[g].at[order, part, j - 1]
                st[g, 1, part] = sends(g, 1, part, pairs, b)

        def stage2(g):
            base, rows, size, c1, c2 = GROUPS[g]
            for part, (a, b, c) in enumerate(order_axes):
                done(g, 1, part)
                r = r2[g]
                own = p2[g][order, part, pl.ds(pl.multiple_of(pos[b] * c2, 8), c2), :]
                p3[g][order, part] = own + r[order, part, 0] + r[order, part, 1] + r[order, part, 2]

                def pairs(j):
                    return p3[g].at[order, part], r3[g].at[order, part, j - 1]
                st[g, 2, part] = sends(g, 2, part, pairs, c)

        def stage3(g):
            base, rows, size, c1, c2 = GROUPS[g]
            for part, (a, b, c) in enumerate(order_axes):
                done(g, 2, part)
                r = r3[g]
                total = (p3[g][order, part] + r[order, part, 1]) + (r[order, part, 0] + r[order, part, 2])
                at = pl.ds(pl.multiple_of(part * size + pos[a] * c1 + pos[b] * c2, c2), c2)
                if g == 0:
                    n = part * 4 + pos[a]
                    first = lax.broadcasted_iota(jnp.int32, (c2, BLK), 0) + pos[b] * c2
                    ahead = lax.broadcasted_iota(jnp.int32, (c2, BLK), 1) == lax.rem(first + BLK - 1, BLK)
                    on = (n == 0) | (n == 4) | (n == 7) | (n == 9)
                    low = total - total.astype(bf16).astype(f32)
                    total = jnp.where(ahead & on, pltpu.roll(low, BLK - 1, 1), total)
                fin[g][order, at, :] = total.astype(fin[g].dtype)

                def pairs(j):
                    return fin[g].at[order, at], fin[g].at[order, at]
                st[g, 3, part] = sends(g, 3, part, pairs, b)

        def stage4(g):
            base, rows, size, c1, c2 = GROUPS[g]
            for part, (a, b, c) in enumerate(order_axes):
                done(g, 3, part)
                at = pl.ds(pl.multiple_of(part * size + pos[a] * c1, c1), c1)

                def pairs(j):
                    return fin[g].at[order, at], fin[g].at[order, at]
                st[g, 4, part] = sends(g, 4, part, pairs, a)

        stage0(0)
        put_cross(tot, dot_tn(half(core), u[1]))
        stage0(1)
        if order == 0:
            shares = share_quarter()
            rest()
        else:
            for cp in shares:
                cp.wait()
            shares = share_half()
            rows = pl.ds(pl.multiple_of(ch * Q, Q), Q)
            nf[rows, :] = u[0]
            ns[rows, :] = u[1]
            for cp in shares:
                cp.wait()
        stage1(0)
        if order == 1:
            advance(lax.rem(ch + 1, 4))
        stage1(1)
        stage2(0)
        if order == 1:
            advance(lax.rem(ch + 2, 4))
        stage2(1)
        stage3(0)
        stage3(1)
        stage4(0)
        if order == 1:
            advance(lax.rem(ch + 3, 4))
        for part in range(3):
            done(0, 4, part)
        stage4(1)
        if order == 0:
            for cp in shares:
                cp.wait()
            shares = send_half()

        square = jnp.zeros((BLK, BLK), f32)
        whole_d, rows_d, cols_d = [], [], []
        for n, (i, j) in enumerate(TRI):
            blk = fin[0][order, pl.ds(n * BLK, BLK), :].astype(f32)
            if i == j:
                only = jnp.where(eye, blk + pltpu.roll(blk, 1, 1), 0.0)
                upper = jnp.where(kept, blk, 0.0)
                square = square + (only * only + 2.0 * (upper * upper))
                rows_d.append(jnp.sum(only, axis=0, keepdims=True))
                cols_d.append(jnp.sum(only, axis=1, keepdims=True))
                emat[pl.ds(i * BLK, BLK), pl.ds(j * BLK, BLK)] = upper + upper.T
            else:
                square = square + 2.0 * (blk * blk)
                emat[pl.ds(i * BLK, BLK), pl.ds(j * BLK, BLK)] = blk
                emat[pl.ds(j * BLK, BLK), pl.ds(i * BLK, BLK)] = blk.T
        scale = lax.rsqrt(jnp.sum(square, keepdims=True) + 1e-06)
        dr = jnp.concatenate(rows_d, axis=1) * scale
        dc = jnp.concatenate(cols_d, axis=0) * scale

        def set_diagonal(ref, value):
            for i in range(4):
                at = pl.ds(i * BLK, BLK)
                ref[at, at] = jnp.where(eye, value[:, i * BLK:(i + 1) * BLK], ref[at, at])

        def clear_diagonal(ref):
            for i in range(4):
                at = pl.ds(i * BLK, BLK)
                ref[at, at] = jnp.where(eye, 0.0, ref[at, at])

        e = emat[...] * scale
        xmat[...] = -e
        set_diagonal(xmat, 2.0 - dr)
        for k in range(NSTEPS - 1):
            eb = e.astype(bf16)
            if k > 0:
                xv = xmat[...]
                xmat[...] = xv * (2.0 - dr) - dot_nn(xv.astype(bf16), eb)
            te = dot_nn(eb, eb)
            tr, tc = diagonal(te)
            emat[...] = e * ((2.0 - dc) - dr) - te
            clear_diagonal(emat)
            e = emat[...]
            dr, dc = 2.0 * dr - dr * dr - tr, 2.0 * dc - dc * dc - tc
            if k == 2:
                for part in range(3):
                    done(1, 4, part)
                swap = remote(
                    fin[1].at[order, pl.ds(0, HALF)], far_half.at[order],
                    d_ssem.at[order, 2], d_rsem.at[order, 2], partner,
                )
                swap.start()
        xv = xmat[...]
        xmat[...] = xv * (2.0 - dr) - dot_nn(xv.astype(bf16), e.astype(bf16))
        swap.wait()

        @pl.when(core == 0)
        def _():
            for n in range(8):
                i, j = n // 4, n % 4
                blk = fin[1][order, pl.ds(n * BLK, BLK), :]
                zmat[pl.ds(j * BLK, BLK), pl.ds(i * BLK, BLK)] = blk.T
                blk = far_half[order, pl.ds(n * BLK, BLK), :]
                zmat[pl.ds(j * BLK, BLK), pl.ds((2 + i) * BLK, BLK)] = blk.T

        @pl.when(core == 1)
        def _():
            for n in range(8):
                i, j = n // 4, n % 4
                blk = fin[1][order, pl.ds(n * BLK, BLK), :]
                zmat[pl.ds((2 + i) * BLK, BLK), pl.ds(j * BLK, BLK)] = blk
                blk = far_half[order, pl.ds(n * BLK, BLK), :]
                zmat[pl.ds(i * BLK, BLK), pl.ds(j * BLK, BLK)] = blk

        zrows = pl.ds(0, C) if order == 0 else pl.ds(pl.multiple_of(y_lo * 2 * W, 2 * W), 2 * W)
        zv = zmat[zrows, :]
        zh = zv.astype(bf16)
        zl = (zv - zh.astype(f32)).astype(bf16)
        xv = xmat[...]
        xh = xv.astype(bf16)
        xl = (xv - xh.astype(f32)).astype(bf16)
        prod = dot_nn(zh, xh) + (dot_nn(zh, xl) + dot_nn(zl, xh))
        amat[order, core, zrows, :] = (prod * (-scale)).astype(bf16)
        if order == 0:
            part_rows = pl.ds(0, C)
        else:
            part_rows = pl.ds(pl.multiple_of((y_lo * 2 + 1 - core) * W, W), W)
        swap = remote(
            amat.at[order, core, part_rows], amat.at[order, core, part_rows],
            d_ssem.at[order, 3], d_rsem.at[order, 3], partner,
        )
        swap.start()
        swap.wait()
        if order == 0:
            new_f = u[0].astype(f32) + dot_nt(s1buf[...], amat[order, 1])
            new_b = s2buf[...].astype(f32) + dot_nt(g1buf[...], amat[order, 0])
            u[0] = new_f.astype(bf16)
            u[1] = new_b.astype(bf16)

    for t in range(4):
        rows = pl.ds(t * Q, Q)
        out_f[rows, :] = (nf[rows, mycols].astype(f32) + dot_nt(ns[rows, :], amat[1, 1, mycols, :])).astype(bf16)
        out_b[rows, :] = (ns[rows, mycols].astype(f32) + dot_nt(nf[rows, :], amat[1, 0, mycols, :])).astype(bf16)


def local(fwd_in, bwd_in):
    vmem = pl.BlockSpec(memory_space=pltpu.VMEM)
    hbm = pl.BlockSpec(memory_space=pltpu.HBM)
    rows = fwd_in.shape[0]
    dma = pltpu.SemaphoreType.DMA
    return pl.pallas_call(
        kernel,
        out_shape=(jax.ShapeDtypeStruct((rows, W), bf16), jax.ShapeDtypeStruct((rows, W), bf16)),
        in_specs=[hbm, hbm],
        out_specs=(vmem, vmem),
        scratch_shapes=[
            pltpu.VMEM((HALO + rows, C), bf16),
            pltpu.VMEM((HALO + rows, C), bf16),
            pltpu.VMEM((HALO, C), bf16),
            pltpu.VMEM((HALO, C), bf16),
            pltpu.VMEM((Q + HALO, C), f32),
            pltpu.VMEM((2, Q, C), bf16),
            pltpu.VMEM((Q, C), bf16),
            pltpu.VMEM((Q, C), bf16),
            pltpu.VMEM((Q, C), bf16),
            pltpu.VMEM((rows, C), bf16),
            pltpu.VMEM((rows, C), bf16),
            pltpu.VMEM((ORDERS, ROWS, BLK), NEAR),
            pltpu.VMEM((ORDERS, ROWS, BLK), NEAR),
            pltpu.VMEM((ROWS, BLK), f32),
            pltpu.VMEM((ORDERS, ROWS, BLK), FIRST),
            pltpu.VMEM((ORDERS, 3, 3, 128, BLK), FIRST),
            pltpu.VMEM((ORDERS, 3, 3, 96, BLK), FIRST),
            pltpu.VMEM((ORDERS, 3, 128, BLK), f32),
            pltpu.VMEM((ORDERS, 3, 96, BLK), f32),
            pltpu.VMEM((ORDERS, 3, 3, 32, BLK), f32),
            pltpu.VMEM((ORDERS, 3, 3, 24, BLK), f32),
            pltpu.VMEM((ORDERS, 3, 32, BLK), f32),
            pltpu.VMEM((ORDERS, 3, 24, BLK), f32),
            pltpu.VMEM((ORDERS, 3, 3, 32, BLK), f32),
            pltpu.VMEM((ORDERS, 3, 3, 24, BLK), f32),
            pltpu.VMEM((ORDERS, 1536, BLK), bf16),
            pltpu.VMEM((ORDERS, 1152, BLK), f32),
            pltpu.VMEM((ORDERS, HALF, BLK), f32),
            pltpu.VMEM((C, C), f32),
            pltpu.VMEM((C, C), f32),
            pltpu.VMEM((C, C), f32),
            pltpu.VMEM((ORDERS, 2, C, C), bf16),
            dma((2,)), dma((2, 3)), dma((2, 3)), dma((2, 4)), dma((2, 3)), dma((2,)),
            dma((2, 4)), dma((2, 4)), dma((2, 3)), dma((2, 3)),
            dma((ORDERS, 4)), dma((ORDERS, 4)),
            dma((ORDERS, 2, 5, 3, 3)), dma((ORDERS, 2, 5, 3, 3)),
        ],
        compiler_params=pltpu.CompilerParams(
            collective_id=0, has_side_effects=True, vmem_limit_bytes=56 * 1024 * 1024
        ),
        name="lattice",
    )(fwd_in, bwd_in)


def solution(mesh):
    in_specs = (P("tm", "chan"), P("tm", "chan"))
    out_specs = (P("tm", "chan"), P("tm", "chan"))
    return jax.shard_map(local, mesh=mesh, in_specs=in_specs, out_specs=out_specs, check_vma=False)
```
